512 devices in a mesh: space: 64 (over z, x_lo, core), shot: 8 (over x_hi, y).
Axes of the slice: x: 4 (x_hi: 2, x_lo: 2; x = x_hi * 2 + x_lo), y: 4, z: 16, core: 2. Of those that a mesh axis runs over, the one named last changes fastest.
Arguments:
- courant: float32 [1024, 64, 128], P('space'), may hold values from 0.15 to 0.42
- p_current: float32 [8, 1024, 64, 128], P('shot', 'space'), may hold values from -6 to 6
- p_later: float32 [8, 1024, 64, 128], P('shot', 'space'), may hold values from -6 to 6
- q_current: float32 [8, 1024, 64, 128], P('shot', 'space'), may hold values from -6 to 6
- q_later: float32 [8, 1024, 64, 128], P('shot', 'space'), may hold values from -6 to 6
- wavelet: float32 [8, 6], P('shot'), may hold values from -24 to 24
- source_cell: int32 [8], P('shot'), may hold values from 0 to 8388607
- receiver_cells: int32 [8, 256], P('shot'), may hold values from 0 to 8388607
- residual_data: float32 [8, 6, 256], P('shot'), may hold values from -6 to 6
Outputs:
- gradient: float32 [1024, 64, 128], P('space', 'shot')
- q_final: float32 [8, 1024, 64, 128], P('shot', 'space')
The draws below stay inside these ranges and needn't reach their ends.
Inputs may be any that keep to these rules, and one draw needn't show every extreme that they name: `source_cell`: a flat cell index of the whole grid. `receiver_cells`: flat cell indices of the whole grid; cells may repeat.
All inputs are finite; a program needn't handle non-finite values.
Results may differ from the reference program's by a relative error of at most 0.0003.
Values sent between devices are 32-bit elements; how exact they have to be, the bound alone decides.
No kernel may reach another device: no remote copies, remote signals or barrier semaphores. Data moves between devices by JAX's collectives and lax.ppermute only.
A program may use at most 64 MiB of HBM per device.

```python
import math
import jax
import jax.numpy as jnp
from jax import lax

NY = 64
NZ = 128
STEPS = 6
REC = 256
NX = 1024
SHOTS = 8


def set_ends(result, key, low, high):
    spot = [jax.random.randint(jax.random.fold_in(key, axis), (), 0, length) for axis, length in enumerate(result.shape)]
    longest = result.shape.index(max(result.shape))
    next_to = spot[:longest] + [(spot[longest] + 1) % result.shape[longest]] + spot[longest + 1:]
    return result.at[tuple(spot)].set(low).at[tuple(next_to)].set(high)


def steps_of(rng, shape, shards, low, top_value):
    level, own = 1.0, jax.random.fold_in(rng, 6)
    for dim, blocks in shards:
        steps = jnp.exp(jax.random.uniform(jax.random.fold_in(own, dim), (blocks,), jnp.float32, low / len(shards), top_value / len(shards)))
        level = level * jnp.repeat(steps, shape[dim] // blocks).reshape([-1 if axis == dim else 1 for axis in range(len(shape))])
    return level


def scatter_about(rng, shape, scale, reach, cuts=(), held_as=jnp.bfloat16):
    drawn = jax.random.normal(rng, shape, jnp.float32) * scale
    if len(cuts) > 0:
        drawn = steps_of(rng, shape, cuts, -0.22, 0.18) * drawn
    return jnp.clip(drawn, min=-reach, max=reach).astype(held_as)


def setup_inputs(seed: int = 0) -> dict:
    arg_keys = jax.random.split(jax.random.key(seed), 10)
    courant = jnp.clip(jnp.exp(math.log(0.42) - 1.0296193 * jax.random.uniform(arg_keys[0], (NX, NY, NZ), jnp.float32) ** steps_of(arg_keys[0], (NX, NY, NZ), ((0, 64),), -0.2, 0.2)), 0.15, 0.42)
    p_current = scatter_about(arg_keys[1], (SHOTS, NX, NY, NZ), 1.0, 6.0, ((0, 8), (1, 64)), jnp.float32)
    p_later = scatter_about(arg_keys[2], (SHOTS, NX, NY, NZ), 1.0, 6.0, ((0, 8), (1, 64)), jnp.float32)
    q_current = scatter_about(arg_keys[3], (SHOTS, NX, NY, NZ), 1.0, 6.0, ((0, 8), (1, 64)), jnp.float32)
    q_later = scatter_about(arg_keys[4], (SHOTS, NX, NY, NZ), 1.0, 6.0, ((0, 8), (1, 64)), jnp.float32)
    wavelet = scatter_about(arg_keys[5], (SHOTS, STEPS), 4.0, 24.0, ((0, 8),), jnp.float32)
    source_cell = set_ends(jax.random.randint(arg_keys[6], (SHOTS,), 0, NX * NY * NZ), jax.random.fold_in(arg_keys[6], 1), 0, (NX * NY * NZ) - 1).astype(jnp.int32)
    receiver_cells = set_ends(jax.random.randint(arg_keys[7], (SHOTS, REC), 0, NX * NY * NZ), jax.random.fold_in(arg_keys[7], 1), 0, (NX * NY * NZ) - 1).astype(jnp.int32)
    residual_data = scatter_about(arg_keys[8], (SHOTS, STEPS, REC), 1.0, 6.0, ((0, 8),), jnp.float32)
    return dict(courant=courant, p_current=p_current, p_later=p_later, q_current=q_current, q_later=q_later, wavelet=wavelet, source_cell=source_cell, receiver_cells=receiver_cells, residual_data=residual_data)


coefs = (-205.0 / 72.0, 8.0 / 5.0, -1.0 / 5.0, 8.0 / 315.0, -1.0 / 560.0)


def laplace_rows(field):
    extent = field.shape[0]
    core = field[4:extent - 4]
    total = 3.0 * coefs[0] * core
    for j in range(1, 5):
        total = total + coefs[j] * (field[4 + j:extent - 4 + j] + field[4 - j:extent - 4 - j])
    width_y = core.shape[1]
    padded_y = jnp.pad(core, ((0, 0), (4, 4), (0, 0)))
    for j in range(1, 5):
        total = total + coefs[j] * (padded_y[:, 4 + j:4 + j + width_y] + padded_y[:, 4 - j:4 - j + width_y])
    width_z = core.shape[2]
    padded_z = jnp.pad(core, ((0, 0), (0, 0), (4, 4)))
    for j in range(1, 5):
        total = total + coefs[j] * (padded_z[:, :, 4 + j:4 + j + width_z] + padded_z[:, :, 4 - j:4 - j + width_z])
    return total


def laplace_whole(field):
    return laplace_rows(jnp.pad(field, ((4, 4), (0, 0), (0, 0))))


def inject_cells(field, cells, values):
    flat = field.reshape(-1)
    flat = flat.at[cells.astype(jnp.int32)].add(values)
    return flat.reshape(field.shape)


def reference(courant, p_current, p_later, q_current, q_later, wavelet, source_cell, receiver_cells, residual_data):
    speed2 = courant * courant

    def one_shot(total, items):
        pc, pn, qc, qn, wave, source, receivers, residual = items
        grad = jnp.zeros(pc.shape, jnp.float32)
        for k in range(STEPS):
            lp = laplace_whole(pc)
            lq = laplace_whole(qc)
            grad = grad + qc * lp
            p_new = inject_cells(2.0 * pc - pn + speed2 * lp, source[None], wave[k][None])
            q_new = inject_cells(2.0 * qc - qn + speed2 * lq, receivers, residual[k])
            pn, pc = pc, p_new
            qn, qc = qc, q_new
        return total + grad, qc

    start = jnp.zeros(courant.shape, jnp.float32)
    summed, q_final = lax.scan(one_shot, start, (p_current, p_later, q_current, q_later, wavelet, source_cell, receiver_cells, residual_data))
    gradient = summed * (1.0 / (STEPS * SHOTS))
    return gradient, q_final
```

```python
import functools
import jax
import jax.numpy as jnp
from jax import lax
from jax.experimental import pallas as pl
from jax.experimental.pallas import tpu as pltpu
from jax.sharding import PartitionSpec as P

STEPS = 6
SCALE = 5040.0
MIDDLE = -14350.0
COEFS = (None, 8064.0, -1008.0, 128.0, -9.0)
PAD = 8
HALO = 8
F32 = jnp.float32

VM = pl.BlockSpec(memory_space=pltpu.VMEM)
SM = pl.BlockSpec(memory_space=pltpu.SMEM)
ANY = pl.BlockSpec(memory_space=pltpu.HBM)


def on_chip(*shape, dtype=F32):
    return pltpu.VMEM(shape, dtype)


def off_chip(value):
    return pltpu.with_memory_space_constraint(value, pltpu.HBM)


def keep(value):
    return pltpu.with_memory_space_constraint(value, pltpu.VMEM)


def params(mib):
    return pltpu.CompilerParams(vmem_limit_bytes=mib << 20)


def cost(us):
    return pl.CostEstimate(flops=int(us * 4e6), bytes_accessed=1 << 20, transcendentals=0)


def pack_kernel(info, pc, pn, qc, qn, speed, near, far, sem):
    rows = speed.shape[0]
    odd = info[1]
    copies = []
    for out, low in ((near, odd), (far, 1 - odd)):
        high = 1 - low
        at = 0
        for src, count in ((pc.at[0], 8), (qc.at[0], 8), (pn.at[0], 4), (qn.at[0], 4), (speed, 4)):
            copies.append(
                pltpu.make_async_copy(
                    src.at[pl.ds(high * (rows - count), count)], out.at[pl.ds(at, count)], sem.at[len(copies)]
                )
            )
            at += count
    for c in copies:
        c.start()
    for c in copies:
        c.wait()


def pack(info, *fields):
    ny, nz = fields[0].shape[2:]
    return pl.pallas_call(
        pack_kernel,
        out_shape=(on_chip(28, ny, nz),) * 2,
        in_specs=[SM] + [ANY] * 5,
        out_specs=(VM,) * 2,
        scratch_shapes=[pltpu.SemaphoreType.DMA((10,))],
        compiler_params=params(4),
        cost_estimate=cost(1.0),
        name="pack",
    )(info, *[off_chip(a) for a in fields])


def load_kernel(info, cells, pc, pn, qc, qn, speed, up, vp, uq, vq, s2, count, order, sem):
    rows, ny = pc.shape[1:3]
    pairs = [
        (src.at[0], dst.at[pl.ds(HALO, rows), pl.ds(PAD, ny)])
        for src, dst in ((pc, up), (pn, vp), (qc, uq), (qn, vq))
    ]
    pairs.append((speed, s2.at[pl.ds(HALO, rows)]))
    copies = [pltpu.make_async_copy(src, dst, sem.at[i]) for i, (src, dst) in enumerate(pairs)]
    for c in copies:
        c.start()
    ext, wide, nz = up.shape
    zero = jnp.zeros((PAD, nz), F32)

    def clear(r, _):
        for ref in (up, vp, uq, vq):
            ref[r, 0:PAD, :] = zero
            ref[r, PAD + ny : wide, :] = zero
        return 0

    lax.fori_loop(0, ext, clear, 0)
    low = (info[0] - 4) * (ny * nz)
    span = (rows + 8) * (ny * nz)

    def find(i, n):
        for j in range(8):
            at = cells[0, i * 8 + j] - low
            order[n] = i * 8 + j
            n = n + jnp.where((at >= 0) & (at < span), 1, 0)
        return n

    count[0] = lax.fori_loop(0, cells.shape[1] // 8, find, 0)
    for c in copies:
        c.wait()

    def square(r, _):
        s2[r] = (s2[r] * s2[r]) * (1.0 / SCALE)
        return 0

    lax.fori_loop(HALO, HALO + rows, square, 0)


def load(info, cells, *fields):
    rows, ny, nz = fields[-1].shape
    ext, wide = rows + 2 * HALO, ny + 2 * PAD
    field = on_chip(ext, wide, nz)
    return pl.pallas_call(
        load_kernel,
        out_shape=(field,) * 4
        + (
            on_chip(ext, ny, nz),
            jax.ShapeDtypeStruct((1,), jnp.int32),
            jax.ShapeDtypeStruct((cells.shape[1] + 8,), jnp.int32),
        ),
        in_specs=[SM, SM] + [ANY] * 5,
        out_specs=(VM,) * 5 + (SM, SM),
        scratch_shapes=[pltpu.SemaphoreType.DMA((5,))],
        compiler_params=params(16),
        cost_estimate=cost(3.0),
        name="load",
    )(info, cells, *[off_chip(f) for f in fields])


GROUP = 2


def fill_weights(weights):
    depth, nz = weights.shape
    gap = lax.broadcasted_iota(jnp.int32, (depth, nz), 0) % nz - lax.broadcasted_iota(jnp.int32, (depth, nz), 1)
    gap = jnp.abs(gap)
    band = jnp.zeros((depth, nz), F32)
    for j in range(1, 5):
        band = jnp.where(gap == j, COEFS[j], band)
    weights[...] = band.astype(jnp.bfloat16)


def along_z(fields, r, weights):
    wide, nz = fields[0].shape[1:]
    ny = wide - 2 * PAD
    parts = []
    for u in fields:
        core = u[pl.ds(r, GROUP), PAD : PAD + ny, :].reshape(GROUP * ny, nz)
        lead = core.astype(jnp.bfloat16)
        rest = (core - lead.astype(F32)).astype(jnp.bfloat16)
        parts.append(jnp.concatenate([lead, rest], axis=1))
    both = jnp.concatenate(parts, axis=0)
    out = jnp.dot(both, weights[...], preferred_element_type=F32)
    return out.reshape(len(fields), GROUP, ny, nz)


def laplace(u, r, z):
    ny = u.shape[1] - 2 * PAD
    core = u[r, PAD : PAD + ny, :]
    total = (3.0 * MIDDLE) * core
    for j in range(1, 5):
        pair = u[r + j, PAD : PAD + ny, :] + u[r - j, PAD : PAD + ny, :]
        pair = pair + (u[r, PAD + j : PAD + j + ny, :] + u[r, PAD - j : PAD - j + ny, :])
        total = total + COEFS[j] * pair
    return core, total + z


def place(u, low, cell, value, start, count):
    ny, nz = u.shape[1] - 2 * PAD, u.shape[2]
    at = cell - low
    r, y, z = at // (ny * nz) + 4, (at // nz) % ny, at % nz
    lane = lax.broadcasted_iota(jnp.int32, (1, nz), 1)
    hit = (lane == z) & (r >= start) & (r < start + count)
    spot = u.at[r, pl.ds(y + PAD, 1), :]
    spot[...] = spot[...] + jnp.where(hit, value, 0.0)


def side_kernel(block, blocks, far, n_in, *refs):
    first_block, last_block = block == 0, block == blocks - 1
    info, wave, source, cells, values, count, order, arrived = refs[:8]
    s2 = refs[12]
    outs = list(refs[n_in:])
    weights = outs.pop()
    sem = outs.pop() if last_block and far else None
    up, vp, uq, vq = (outs.pop(0) for _ in range(4))
    if first_block:
        s2 = outs.pop(0)
    g = outs.pop(0)
    if last_block and far:
        g[...] = refs[13][...]
    ext, ny, nz = up.shape[0], up.shape[1] - 2 * PAD, up.shape[2]
    own = ext - 2 * HALO
    parts = g.shape[0]
    odd = info[1]
    high = odd if far else 1 - odd
    base = (info[0] - 4) * (ny * nz)
    fill_weights(weights)

    edge, edge4 = high * (ext - 8), 4 + high * (ext - 12)

    def eight(i, _):
        up[edge + i, PAD : PAD + ny, :] = arrived[i]
        uq[edge + i, PAD : PAD + ny, :] = arrived[8 + i]
        return 0

    lax.fori_loop(0, 8, eight, 0, unroll=2)
    if first_block:

        def four(i, _):
            vp[edge4 + i, PAD : PAD + ny, :] = arrived[16 + i]
            vq[edge4 + i, PAD : PAD + ny, :] = arrived[20 + i]
            s2[edge4 + i] = (arrived[24 + i] * arrived[24 + i]) * (1.0 / SCALE)
            return 0

        lax.fori_loop(0, 4, four, 0)

    def step(t, pu, pv, qu, qv, begin, rows, mine):
        def trip(i, _):
            r = begin + i * GROUP
            z = along_z((pu, qu), r, weights)
            for j in range(GROUP):
                speed = s2[r + j]
                core, lap = laplace(pu, r + j, z[0, j])
                if pv is not None:
                    pv[r + j, PAD : PAD + ny, :] = 2.0 * core - pv[r + j, PAD : PAD + ny, :] + speed * lap
                core, total = laplace(qu, r + j, z[1, j])
                qv[r + j, PAD : PAD + ny, :] = 2.0 * core - qv[r + j, PAD : PAD + ny, :] + speed * total
                if mine:
                    term = (core * lap).reshape(parts, ny // parts, nz)
                    if not (first_block and t == 0):
                        term = term + g[:, r + j - HALO]
                    g[:, r + j - HALO] = term
            return 0

        lax.fori_loop(0, rows // GROUP, trip, 0)

    def inject(p, q, k, start, rows):
        cell = source[0]
        if p is not None:

            @pl.when((cell >= base) & (cell < base + (own + 8) * (ny * nz)))
            def _():
                place(p, base, cell, wave[0, k], start, rows)

        def one(n, _):
            i = order[n]
            place(q, base, cells[0, i], values[0, k, i], start, rows)
            return 0

        lax.fori_loop(0, count[0], one, 0)

    k = 2 * block
    if far:
        start, rows, mine = 4 + 16 * high, 8, (8 + 12 * high, 4)
    else:
        start, rows, mine = 4 + 8 * high, 16, (8 + 4 * high, 12)
    step(0, up, vp, uq, vq, 4 + 20 * high, 4, False)
    step(0, up, vp, uq, vq, *mine, True)
    inject(vp, vq, k, start, rows)
    half = 8 + 8 * high
    step(1, vp, None if last_block else up, vq, uq, half, 8, True)
    inject(None if last_block else up, uq, k + 1, half, 8)
    if not last_block:
        (send,) = outs

        def out(i, _):
            send[i] = up[half + i, PAD : PAD + ny, :]
            send[8 + i] = uq[half + i, PAD : PAD + ny, :]
            return 0

        lax.fori_loop(0, 8, out, 0, unroll=2)
    elif far:
        (final,) = outs
        done = pltpu.make_async_copy(uq.at[pl.ds(HALO, own), pl.ds(PAD, ny)], final.at[0], sem)
        done.start()
        done.wait()


def side(block, blocks, far, parts, scalars, arrived, fields, s2, g):
    first_block, last_block = block == 0, block == blocks - 1
    ext, ny, nz = s2.shape
    own = ext - 2 * HALO
    end = last_block and far
    args = [*scalars, keep(arrived), *[keep(f) for f in fields], keep(s2)]
    field = on_chip(*fields[0].shape)
    outs, alias = [field] * 4, {8: 0, 9: 1, 10: 2, 11: 3}
    if first_block:
        alias[12] = 4
        outs.append(on_chip(*s2.shape))
    if g is not None:
        args.append(keep(g))
        if not end:
            alias[13] = len(outs)
    outs.append(jax.ShapeDtypeStruct((parts, own, ny // parts, nz), F32) if end else on_chip(parts, own, ny // parts, nz))
    specs = [VM] * len(outs)
    scratch = [pltpu.VMEM((2 * nz, nz), jnp.bfloat16)]
    if not last_block:
        outs.append(on_chip(16, ny, nz))
        specs.append(VM)
    elif far:
        outs.append(jax.ShapeDtypeStruct((1, own, ny, nz), F32))
        specs.append(ANY)
        scratch.insert(0, pltpu.SemaphoreType.DMA)
    res = list(
        pl.pallas_call(
            functools.partial(side_kernel, block, blocks, far, len(args)),
            out_shape=tuple(outs),
            in_specs=[SM] * 7 + [VM] * (len(args) - 7),
            out_specs=tuple(specs),
            scratch_shapes=scratch,
            input_output_aliases=alias,
            compiler_params=params(16),
            cost_estimate=cost(4.0),
            name=("far" if far else "near") + f"{block}",
        )(*args)
    )
    fields = res[:4]
    if first_block:
        s2 = res.pop(4)
    return fields, s2, res[4], res[5] if len(res) > 5 else None


def swap_near(value, axis):
    return lax.ppermute(value, axis, [(i, i ^ 1) for i in range(lax.axis_size(axis))])


def swap_far(value, axis):
    count = lax.axis_size(axis)
    return lax.ppermute(value, axis, [(i, i + 1 if i % 2 else i - 1) for i in range(1, count - 1)])


def body(courant, p_current, p_later, q_current, q_later, wavelet, source_cell, receiver_cells, residual_data):
    rows = courant.shape[0]
    shots = lax.axis_size("shot")
    blocks = STEPS // 2
    index = lax.axis_index("space").astype(jnp.int32)
    info = jnp.stack([index * rows, index % 2])
    near, far = pack(info, p_current, p_later, q_current, q_later, courant)
    near = swap_near(near, "space")
    far = swap_far(far, "space")
    *fields, s2, count, order = load(info, receiver_cells, p_current, p_later, q_current, q_later, courant)
    scalars = (info, wavelet, source_cell, receiver_cells, residual_data, count, order)
    g = None
    for b in range(blocks):
        last = b == blocks - 1
        fields, s2, g, out = side(b, blocks, False, shots, scalars, near, fields, s2, g)
        if not last:
            near = swap_near(out, "space")
        fields, s2, g, out = side(b, blocks, True, shots, scalars, far, fields, s2, g)
        if not last:
            far = swap_far(out, "space")
    arrived = lax.all_to_all(g, "shot", split_axis=0, concat_axis=0, tiled=True)
    gradient = arrived.sum(axis=0) * (1.0 / (SCALE * STEPS * shots))
    return gradient, out


def solution(mesh):
    in_specs = (
        P("space", None, None),
        P("shot", "space", None, None),
        P("shot", "space", None, None),
        P("shot", "space", None, None),
        P("shot", "space", None, None),
        P("shot", None),
        P("shot"),
        P("shot", None),
        P("shot", None, None),
    )
    out_specs = (P("space", "shot", None), P("shot", "space", None, None))
    return jax.shard_map(body, mesh=mesh, in_specs=in_specs, out_specs=out_specs, check_vma=False)
```

```python
import functools
import jax
import jax.numpy as jnp
from jax import lax
from jax.experimental import pallas as pl
from jax.experimental.pallas import tpu as pltpu
from jax.sharding import PartitionSpec as P

STEPS = 6
SCALE = 5040.0
MIDDLE = -14350.0
COEFS = (None, 8064.0, -1008.0, 128.0, -9.0)
PAD = 8
HALO = 8
F32 = jnp.float32

VM = pl.BlockSpec(memory_space=pltpu.VMEM)
SM = pl.BlockSpec(memory_space=pltpu.SMEM)
ANY = pl.BlockSpec(memory_space=pltpu.HBM)


def on_chip(*shape, dtype=F32):
    return pltpu.VMEM(shape, dtype)


def off_chip(value):
    return pltpu.with_memory_space_constraint(value, pltpu.HBM)


def keep(value):
    return pltpu.with_memory_space_constraint(value, pltpu.VMEM)


def params(mib):
    return pltpu.CompilerParams(vmem_limit_bytes=mib << 20)


def cost(us):
    return pl.CostEstimate(flops=int(us * 4e6), bytes_accessed=1 << 20, transcendentals=0)


def rows_out(high, rows, out, parts, sem, base):
    copies, at = [], 0
    for src, count in parts:
        copies.append(
            pltpu.make_async_copy(
                src.at[pl.ds(high * (rows - count), count)], out.at[pl.ds(at, count)], sem.at[base + len(copies)]
            )
        )
        at += count
    return copies


def pack_kernel(info, pc, pn, qc, qn, speed, near, far, sem):
    rows = speed.shape[0]
    odd = info[1]
    p, q, p_old, q_old = (ref.at[0] for ref in (pc, qc, pn, qn))
    copies = rows_out(1 - odd, rows, near, ((p, 8), (q, 8), (p_old, 4), (q_old, 4), (speed, 4)), sem, 0)
    copies += rows_out(odd, rows, far, ((p, 8), (p_old, 4), (speed, 4)), sem, 5)
    for c in copies:
        c.start()
    for c in copies:
        c.wait()


def pack(info, *fields):
    ny, nz = fields[0].shape[2:]
    return pl.pallas_call(
        pack_kernel,
        out_shape=(on_chip(28, ny, nz), on_chip(16, ny, nz)),
        in_specs=[SM] + [ANY] * 5,
        out_specs=(VM,) * 2,
        scratch_shapes=[pltpu.SemaphoreType.DMA((8,))],
        compiler_params=params(4),
        cost_estimate=cost(1.0),
        name="pack",
    )(info, *[off_chip(a) for a in fields])


def load_kernel(info, cells, values, pc, pn, qc, qn, speed, up, vp, uq, vq, s2, added, weights, far, order, sem):
    rows, ny = pc.shape[1:3]
    pairs = [
        (src.at[0], dst.at[pl.ds(HALO, rows), pl.ds(PAD, ny)])
        for src, dst in ((pc, up), (pn, vp), (qc, uq), (qn, vq))
    ]
    pairs.append((speed, s2.at[pl.ds(HALO, rows)]))
    copies = [pltpu.make_async_copy(src, dst, sem.at[i]) for i, (src, dst) in enumerate(pairs)]
    copies += rows_out(info[1], rows, far, ((qc.at[0], 8), (qn.at[0], 4)), sem, 5)
    for c in copies:
        c.start()
    ext, wide, nz = up.shape
    zero = jnp.zeros((PAD, nz), F32)

    def clear(r, _):
        for ref in (up, vp, uq, vq):
            ref[r, 0:PAD, :] = zero
            ref[r, PAD + ny : wide, :] = zero
        return 0

    lax.fori_loop(0, ext, clear, 0)
    fill_weights(weights)
    steps, near_rows = added.shape[:2]
    blank = jnp.zeros((ny, nz), F32)

    def clear_added(r, _):
        for k in range(steps):
            added[k, r] = blank
        return 0

    lax.fori_loop(0, near_rows, clear_added, 0)
    low = (info[0] - 4) * (ny * nz)
    span = (rows + 8) * (ny * nz)

    def find(i, n):
        for j in range(8):
            at = cells[0, i * 8 + j] - low
            order[n] = i * 8 + j
            n = n + jnp.where((at >= 0) & (at < span), 1, 0)
        return n

    count = lax.fori_loop(0, cells.shape[1] // 8, find, 0)
    lane = lax.broadcasted_iota(jnp.int32, (1, nz), 1)

    def collect(n, _):
        i = order[n]
        at = cells[0, i] - low
        r, y, z = at // (ny * nz), (at // nz) % ny, at % nz
        spots = [added.at[k, r, pl.ds(y, 1), :] for k in range(steps)]
        new = [spot[...] + jnp.where(lane == z, values[0, k, i], 0.0) for k, spot in enumerate(spots)]
        for spot, value in zip(spots, new):
            spot[...] = value
        return 0

    lax.fori_loop(0, count, collect, 0)
    for c in copies:
        c.wait()

    def square(r, _):
        s2[r] = (s2[r] * s2[r]) * (1.0 / SCALE)
        return 0

    lax.fori_loop(HALO, HALO + rows, square, 0)


def load(info, cells, values, *fields):
    rows, ny, nz = fields[-1].shape
    ext, wide = rows + 2 * HALO, ny + 2 * PAD
    field = on_chip(ext, wide, nz)
    return pl.pallas_call(
        load_kernel,
        out_shape=(field,) * 4
        + (
            on_chip(ext, ny, nz),
            on_chip(values.shape[1], rows + 8, ny, nz),
            on_chip(2 * nz, nz, dtype=jnp.bfloat16),
            on_chip(12, ny, nz),
        ),
        in_specs=[SM] * 3 + [ANY] * 5,
        out_specs=(VM,) * 8,
        scratch_shapes=[pltpu.SMEM((cells.shape[1] + 8,), jnp.int32), pltpu.SemaphoreType.DMA((7,))],
        compiler_params=params(16),
        cost_estimate=cost(3.0),
        name="load",
    )(info, cells, values, *[off_chip(f) for f in fields])


GROUP = 4


def fill_weights(weights):
    depth, nz = weights.shape
    gap = lax.broadcasted_iota(jnp.int32, (depth, nz), 0) % nz - lax.broadcasted_iota(jnp.int32, (depth, nz), 1)
    gap = jnp.abs(gap)
    band = jnp.zeros((depth, nz), F32)
    for j in range(1, 5):
        band = jnp.where(gap == j, COEFS[j], band)
    weights[...] = band.astype(jnp.bfloat16)


def along_z(fields, r, weights):
    wide, nz = fields[0].shape[1:]
    ny = wide - 2 * PAD
    parts = []
    for u in fields:
        core = u[pl.ds(r, GROUP), PAD : PAD + ny, :].reshape(GROUP * ny, nz)
        lead = core.astype(jnp.bfloat16)
        rest = (core - lead.astype(F32)).astype(jnp.bfloat16)
        parts.append(jnp.concatenate([lead, rest], axis=1))
    both = jnp.concatenate(parts, axis=0)
    out = jnp.dot(both, weights[...], preferred_element_type=F32)
    return out.reshape(len(fields), GROUP, ny, nz)


def laplace(u, r, z):
    ny = u.shape[1] - 2 * PAD
    core = u[r, PAD : PAD + ny, :]
    total = (3.0 * MIDDLE) * core
    for j in range(1, 5):
        pair = u[r + j, PAD : PAD + ny, :] + u[r - j, PAD : PAD + ny, :]
        pair = pair + (u[r, PAD + j : PAD + j + ny, :] + u[r, PAD - j : PAD - j + ny, :])
        total = total + COEFS[j] * pair
    return core, total + z


def place(u, low, cell, value, start, count):
    ny, nz = u.shape[1] - 2 * PAD, u.shape[2]
    at = cell - low
    r, y, z = at // (ny * nz) + 4, (at // nz) % ny, at % nz
    lane = lax.broadcasted_iota(jnp.int32, (1, nz), 1)
    hit = (lane == z) & (r >= start) & (r < start + count)
    spot = u.at[r, pl.ds(y + PAD, 1), :]
    spot[...] = spot[...] + jnp.where(hit, value, 0.0)


def field_step(u, v, begin, rows, s2, weights, after):
    ny = u[0].shape[1] - 2 * PAD

    def trip(i, _):
        r = begin + i * GROUP
        z = along_z(u, r, weights)
        for j in range(GROUP):
            speed = s2[r + j]
            seen = []
            for n, (now, new) in enumerate(zip(u, v)):
                core, total = laplace(now, r + j, z[n, j])
                more = after(n, r + j, core, total, seen)
                seen.append(total)
                if new is not None:
                    value = 2.0 * core - new[r + j, PAD : PAD + ny, :] + speed * total
                    new[r + j, PAD : PAD + ny, :] = value if more is None else value + more
        return 0

    lax.fori_loop(0, rows // GROUP, trip, 0)


def add_image(g, r, product, fresh):
    parts, _, rest, nz = g.shape
    term = product.reshape(parts, rest, nz)
    g[:, r - HALO] = term if fresh else term + g[:, r - HALO]


def add_source(info, source, wave, k, p, start, rows):
    ext, ny, nz = p.shape[0], p.shape[1] - 2 * PAD, p.shape[2]
    base = (info[0] - 4) * (ny * nz)
    cell = source[0]

    @pl.when((cell >= base) & (cell < base + (ext - 8) * (ny * nz)))
    def _():
        place(p, base, cell, wave[0, k], start, rows)


def rows_in(dst, at, src, start, count):
    ny = src.shape[1]

    def one(i, _):
        dst[at + i, PAD : PAD + ny, :] = src[start + i]
        return 0

    lax.fori_loop(0, count, one, 0, unroll=2)


def speed_in(s2, at, src, start):
    def one(i, _):
        s2[at + i] = (src[start + i] * src[start + i]) * (1.0 / SCALE)
        return 0

    lax.fori_loop(0, 4, one, 0)


def rows_back(send, at, u, start):
    ny = send.shape[1]

    def one(i, _):
        send[at + i] = u[start + i, PAD : PAD + ny, :]
        return 0

    lax.fori_loop(0, 8, one, 0, unroll=2)


def near_kernel(block, blocks, n_in, *refs):
    first_block, last_block = block == 0, block == blocks - 1
    info, wave, source, added, weights, arrived = refs[:6]
    s2 = refs[10]
    outs = list(refs[n_in:])
    up, vp, uq, vq = (outs.pop(0) for _ in range(4))
    if first_block:
        s2 = outs.pop(0)
    g = outs.pop(0)
    ext = up.shape[0]
    high = 1 - info[1]
    edge, edge4 = high * (ext - 8), 4 + high * (ext - 12)
    rows_in(up, edge, arrived, 0, 8)
    rows_in(uq, edge, arrived, 8, 8)
    if first_block:
        rows_in(vp, edge4, arrived, 16, 4)
        rows_in(vq, edge4, arrived, 20, 4)
        speed_in(s2, edge4, arrived, 24)
    k = 2 * block

    def after(t, mine):
        def act(n, r, core, total, seen):
            if n == 0:
                return None
            if mine:
                add_image(g, r, core * seen[0], first_block and t == 0)
            return added[k + t, r - 4]

        return act

    half = 8 + 8 * high
    field_step((up, uq), (vp, vq), 4 + 20 * high, 4, s2, weights, after(0, False))
    field_step((up, uq), (vp, vq), 8 + 4 * high, 12, s2, weights, after(0, True))
    add_source(info, source, wave, k, vp, 4 + 8 * high, 16)
    field_step((vp, vq), (None if last_block else up, uq), half, 8, s2, weights, after(1, True))
    if not last_block:
        add_source(info, source, wave, k + 1, up, half, 8)
        rows_back(outs[0], 0, up, half)
        rows_back(outs[0], 8, uq, half)


def far_p_kernel(block, blocks, n_in, *refs):
    first_block, last_block = block == 0, block == blocks - 1
    info, wave, source, weights, arrived = refs[:5]
    s2 = refs[7]
    outs = list(refs[n_in:])
    u, v = outs.pop(0), outs.pop(0)
    if first_block:
        s2 = outs.pop(0)
    lap = outs.pop(0)
    ext = u.shape[0]
    high = info[1]
    edge4 = 4 + high * (ext - 12)
    rows_in(u, high * (ext - 8), arrived, 0, 8)
    if first_block:
        rows_in(v, edge4, arrived, 8, 4)
        speed_in(s2, edge4, arrived, 12)
    k = 2 * block
    half = 8 + 8 * high

    def after(t, begin):
        def act(n, r, core, total, seen):
            lap[t, r - begin] = total

        return act

    begin = 4 + 16 * high
    field_step((u,), (v,), begin, 8, s2, weights, after(0, begin))
    add_source(info, source, wave, k, v, begin, 8)
    field_step((v,), (None if last_block else u,), half, 8, s2, weights, after(1, half))
    if not last_block:
        add_source(info, source, wave, k + 1, u, half, 8)
        rows_back(outs[0], 0, u, half)


def far_q_kernel(block, blocks, n_in, *refs):
    first_block, last_block = block == 0, block == blocks - 1
    info, added, weights, arrived, _, _, s2, lap = refs[:8]
    outs = list(refs[n_in:])
    u, v, g = outs.pop(0), outs.pop(0), outs.pop(0)
    ext, ny = u.shape[0], u.shape[1] - 2 * PAD
    own = ext - 2 * HALO
    high = info[1]
    rows_in(u, high * (ext - 8), arrived, 0, 8)
    if first_block:
        rows_in(v, 4 + high * (ext - 12), arrived, 8, 4)
    k = 2 * block
    half = 8 + 8 * high
    begin = 4 + 16 * high

    def after(t, low, mine):
        def act(n, r, core, total, seen):
            if mine:
                add_image(g, r, core * lap[t, r - low], first_block and t == 0)
            return added[k + t, r - 4]

        return act

    field_step((u,), (v,), 4 + 20 * high, 4, s2, weights, after(0, begin, False))
    field_step((u,), (v,), 8 + 12 * high, 4, s2, weights, after(0, begin, True))
    field_step((v,), (u,), half, 8, s2, weights, after(1, half, True))
    if last_block:
        final, sem = outs
        done = pltpu.make_async_copy(u.at[pl.ds(HALO, own), pl.ds(PAD, ny)], final.at[0], sem)
        done.start()
        done.wait()
    else:
        rows_back(outs[0], 0, u, half)


def call(kernel, block, blocks, scalars, args, outs, specs, alias, scratch=()):
    n_in = len(scalars) + len(args)
    return list(
        pl.pallas_call(
            functools.partial(kernel, block, blocks, n_in),
            out_shape=tuple(outs),
            in_specs=[SM] * len(scalars) + [VM] * len(args),
            out_specs=tuple(specs),
            scratch_shapes=list(scratch),
            input_output_aliases=alias,
            compiler_params=params(16),
            cost_estimate=cost(3.0),
        )(*scalars, *[keep(a) for a in args])
    )


def near_side(block, blocks, scalars, added, weights, arrived, fields, s2, g, shape):
    ext, ny, nz = s2.shape
    outs, alias = [on_chip(*fields[0].shape)] * 4, {6: 0, 7: 1, 8: 2, 9: 3}
    args = [added, weights, arrived, *fields, s2]
    if block == 0:
        alias[10] = 4
        outs.append(on_chip(ext, ny, nz))
    else:
        alias[11] = 4
        args.append(g)
    outs.append(on_chip(*shape))
    if block < blocks - 1:
        outs.append(on_chip(16, ny, nz))
    res = call(near_kernel, block, blocks, scalars, args, outs, [VM] * len(outs), alias)
    fields = res[:4]
    if block == 0:
        s2 = res.pop(4)
    return fields, s2, res[4], res[5:]


def far_p(block, blocks, scalars, weights, arrived, u, v, s2):
    ext, ny, nz = s2.shape
    outs, alias = [on_chip(*u.shape)] * 2, {5: 0, 6: 1}
    if block == 0:
        alias[7] = 2
        outs.append(on_chip(ext, ny, nz))
    outs.append(on_chip(2, 8, ny, nz))
    if block < blocks - 1:
        outs.append(on_chip(8, ny, nz))
    res = call(far_p_kernel, block, blocks, scalars, [weights, arrived, u, v, s2], outs, [VM] * len(outs), alias)
    if block == 0:
        s2 = res.pop(2)
    return res[0], res[1], s2, res[2], res[3:]


def far_q(block, blocks, info, added, weights, arrived, u, v, s2, lap, g):
    ext, ny, nz = s2.shape
    outs, specs = [on_chip(*u.shape)] * 2 + [on_chip(*g.shape)], [VM] * 3
    scratch = []
    if block < blocks - 1:
        outs.append(on_chip(8, ny, nz))
        specs.append(VM)
    else:
        outs.append(jax.ShapeDtypeStruct((1, ext - 2 * HALO, ny, nz), F32))
        specs.append(ANY)
        scratch.append(pltpu.SemaphoreType.DMA)
    args = [added, weights, arrived, u, v, s2, lap, g]
    return call(far_q_kernel, block, blocks, (info,), args, outs, specs, {4: 0, 5: 1, 8: 2}, scratch)


def swap_near(value, axis):
    return lax.ppermute(value, axis, [(i, i ^ 1) for i in range(lax.axis_size(axis))])


def swap_far(value, axis):
    count = lax.axis_size(axis)
    return lax.ppermute(value, axis, [(i, i + 1 if i % 2 else i - 1) for i in range(1, count - 1)])


def body(courant, p_current, p_later, q_current, q_later, wavelet, source_cell, receiver_cells, residual_data):
    rows = courant.shape[0]
    shots = lax.axis_size("shot")
    blocks = STEPS // 2
    index = lax.axis_index("space").astype(jnp.int32)
    info = jnp.stack([index * rows, index % 2])
    near, p_far = pack(info, p_current, p_later, q_current, q_later, courant)
    near = swap_near(near, "space")
    p_far = swap_far(p_far, "space")
    *fields, s2, added, weights, q_far = load(
        info, receiver_cells, residual_data, p_current, p_later, q_current, q_later, courant
    )
    q_far = swap_far(q_far, "space")
    scalars = (info, wavelet, source_cell)
    shape = (shots, rows, courant.shape[1] // shots, courant.shape[2])
    g = None
    for b in range(blocks):
        last = b == blocks - 1
        fields, s2, g, out = near_side(b, blocks, scalars, added, weights, near, fields, s2, g, shape)
        if not last:
            near = swap_near(out[0], "space")
        up, vp, uq, vq = fields
        up, vp, s2, lap, out = far_p(b, blocks, scalars, weights, p_far, up, vp, s2)
        if not last:
            p_far = swap_far(out[0], "space")
        uq, vq, g, out = far_q(b, blocks, info, added, weights, q_far, uq, vq, s2, lap, g)
        if not last:
            q_far = swap_far(out, "space")
        fields = [up, vp, uq, vq]
    arrived = lax.all_to_all(g, "shot", split_axis=0, concat_axis=0, tiled=True)
    gradient = arrived.sum(axis=0) * (1.0 / (SCALE * STEPS * shots))
    return gradient, out


def solution(mesh):
    in_specs = (
        P("space", None, None),
        P("shot", "space", None, None),
        P("shot", "space", None, None),
        P("shot", "space", None, None),
        P("shot", "space", None, None),
        P("shot", None),
        P("shot"),
        P("shot", None),
        P("shot", None, None),
    )
    out_specs = (P("space", "shot", None), P("shot", "space", None, None))
    return jax.shard_map(body, mesh=mesh, in_specs=in_specs, out_specs=out_specs, check_vma=False)
```
